512 devices in a mesh: groups: 2 (over y), sky: 32 (over z), epoch: 4 (over x), band: 2 (over core).
Axes of the slice: x: 4, y: 2, z: 32, core: 2. Of those that a mesh axis runs over, the one named last changes fastest.
The devices are a block of a 4x8x32 slice.
Arguments:
- slot_pixels: bfloat16 [12288, 6, 32, 512], P(('groups', 'sky', 'epoch'), 'band'), parts along dimension 0, may hold values from -6 to 6
- slot_tile: int32 [12288, 1], P(('groups', 'sky', 'epoch')), parts along dimension 0, may hold values from 0 to 31; in each aligned block of 48 rows (0 to 47, 48 to 95, ...) at most 2 rows name the same one
- slot_offset: int32 [12288, 2], P(('groups', 'sky', 'epoch')), parts along dimension 0, may hold values from -5 to 5
- slot_frac: bfloat16 [12288, 2], P(('groups', 'sky', 'epoch')), parts along dimension 0, may hold values from 0.049804688 to 0.94921875
- slot_sigma: bfloat16 [12288, 6], P(('groups', 'sky', 'epoch'), 'band'), parts along dimension 0, may hold values from 0.5 to 2
- clip_mask: int32 [12288, 6, 16], P(('groups', 'sky', 'epoch')), parts along dimension 0, may hold values 0 or 1
- slot_count: int32 [256], P(('groups', 'sky', 'epoch')), parts along dimension 0, may hold values from 36 to 48
- template: bfloat16 [6, 2048, 512], P('band', ('groups', 'sky')), parts along dimension 1, may hold values from -6 to 6
- prior_weight: float32 [6, 2048], P('band', ('groups', 'sky')), parts along dimension 1, may hold values from 0.5 to 4
Outputs:
- coadd_image: bfloat16 [6, 2048, 512], P('band', ('groups', 'sky'), 'epoch'), parts along dimension 1
- depth_norm: bfloat16 [6, 2048, 512], P('band', ('groups', 'sky'), 'epoch'), parts along dimension 1
The draws below stay inside these ranges and needn't reach their ends.
There are 2 independent parts, one for each index of `groups`. The reference program is written for one: setup_inputs(seed, part) draws one part's arguments, and reference() takes and returns one part's arrays. A program takes and returns all parts, laid end to end along the dimension named above; each array names one. Nothing has to cross between parts.
Inputs may be any that keep to these rules, and one draw needn't show every extreme that they name: `slot_tile`: among the 48 rows of one reading device no owner is named more than 2 times, a bound that some block reaches. `slot_count`: slots of a reading device at or after its count are padding.
All inputs are finite; a program needn't handle non-finite values. No bound on the sum of `clip_mask` on one device may be relied on, other than what follows from the above.
Results may differ from the reference program's by a relative error of at most 0.014.
Values may be sent and summed in bfloat16 or wider, within the bound.
A program may use at most 64 MiB of HBM per device.

```python
import math
import jax
import jax.numpy as jnp
import numpy as np
from jax import lax

BAND_COUNT = 6
TILE_COLS = 512
ROWS_DEV = 32
MAX_SHIFT = 5
MARGIN = 8
CAPACITY = 2
SLOT_DEV = 48
SLOT_TOTAL = 6144
PATCH_ROWS = 1024
N_SKY = 32
N_EPOCH = 4


def plant(array, key, least, high):
    longest = array.shape.index(max(array.shape))
    spots = []
    for shift in (0, 1):
        where = [jax.random.randint(jax.random.fold_in(key, axis), (), 0, length) for axis, length in enumerate(array.shape)]
        where[longest] = (where[longest] + shift) % array.shape[longest]
        spots.append(tuple(where))
    return array.at[spots[0]].set(least).at[spots[1]].set(high)


def block_levels(own_key, extent, shards, smallest, high):
    level = 1.0
    for position, parts in shards:
        steps = jax.random.uniform(jax.random.fold_in(jax.random.fold_in(own_key, 6), position), (parts,), jnp.float32, smallest / len(shards), high / len(shards))
        level = level * jnp.repeat(jnp.exp(steps), extent[position] // parts).reshape((-1,) + (1,) * (len(extent) - 1 - position))
    return level


def shared_out(stream_key, own, number, rows, amount, top, most, skew):
    sequence = jax.random.permutation(stream_key, amount)
    heavy_load, usual = portions_of(amount, rows * top, most, skew, True), portions_of(amount, rows * top, most, skew, False)
    places = jnp.arange(amount)

    def named(lengths, offset_by):
        used = int((lengths > 0).sum())
        fixed = max(1, used // 4)
        moved = fixed + (places - fixed + offset_by * (used - fixed)) % max(1, amount - fixed)
        return jnp.zeros((amount,), jnp.int32).at[sequence[jnp.where(places < fixed, places, moved)]].set(jnp.asarray(lengths, jnp.int32))

    lengths = jnp.where(number % 4 == 0, named(heavy_load, number // 4), named(usual, number - number // 4 - 1))
    mixed = jax.random.permutation(jax.random.fold_in(own, 3), amount)
    giver, receiver = mixed[0:amount // 2 * 2:2], mixed[1:amount // 2 * 2:2]
    slack = jnp.minimum(lengths[giver] - 1, most - lengths[receiver]) // 2
    slack = jnp.where((giver == sequence[0]) | (receiver == sequence[0]) | (lengths[receiver] == 0), 0, jnp.maximum(slack, 0))
    moved = jax.random.randint(jax.random.fold_in(own, 4), (amount // 2,), 0, 1 << 20) % (slack + 1)
    lengths = lengths.at[giver].add(-moved).at[receiver].add(moved)
    labels = jnp.searchsorted(jnp.cumsum(lengths), jnp.arange(rows * top), side="right").astype(jnp.int32)
    table = labels.reshape(top, rows).T
    table = table[jax.random.permutation(jax.random.fold_in(own, 1), rows)]
    offset_by = jax.random.randint(jax.random.fold_in(own, 2), (rows, 1), 0, top)
    return jnp.take_along_axis(table, (jnp.arange(top)[None, :] + offset_by) % top, axis=1)


def portions_of(amount, total, reach, lean, full):
    loads = [(1 << 20) // math.isqrt(standing ** lean) + 1 for standing in range(1, amount + 1)]
    largest = reach if full else min(reach, max(-(-total // amount), total * loads[0] // sum(loads)))
    least = 1 if total - largest >= amount - 1 else 0
    counts, spare = [largest] + [least] * (amount - 1), total - largest - least * (amount - 1)
    while spare > 0:
        movable = [i for i in range(1, amount) if counts[i] < largest] or [i for i in range(1, amount) if counts[i] < reach]
        pool, left = sum([loads[i] for i in movable]), spare
        for i in movable:
            more = min(reach - counts[i], max(1, left * loads[i] // pool), spare)
            counts[i] = counts[i] + more
            spare = spare - more
    return np.array(counts)


def gaussian(rng, dims, spread, most, cuts=(), kind=jnp.bfloat16):
    result = spread * jax.random.normal(rng, dims, jnp.float32)
    if cuts:
        result = result * block_levels(rng, dims, cuts, -0.22, 0.18)
    return jnp.clip(result, -most, most).astype(kind)


def setup_inputs(seed: int = 0, part: int = 0) -> dict:
    splits = jax.random.split(jax.random.key(seed), 10)
    part_splits = jax.random.split(jax.random.fold_in(splits[9], part), 10)
    slot_pixels = gaussian(part_splits[0], (SLOT_TOTAL, BAND_COUNT, ROWS_DEV, TILE_COLS), 1.0, 6.0, ((0, 128), (1, 2)))
    slot_tile_keys = jax.random.split(jax.random.fold_in(part_splits[1], 1), SLOT_TOTAL // SLOT_DEV)
    slot_tile_turns = jax.random.permutation(jax.random.fold_in(part_splits[1], 3), SLOT_TOTAL // SLOT_DEV)
    slot_tile = jax.vmap(lambda own, number: shared_out(jax.random.fold_in(part_splits[1], 2), own, number, SLOT_DEV, N_SKY, 1, CAPACITY, 2))(slot_tile_keys, slot_tile_turns).reshape((SLOT_TOTAL, 1))
    slot_offset = plant(jax.random.randint(part_splits[2], (SLOT_TOTAL, 2), 0 - MAX_SHIFT, MAX_SHIFT + 1), jax.random.fold_in(part_splits[2], 1), 0 - MAX_SHIFT, MAX_SHIFT).astype(jnp.int32)
    slot_frac = jnp.clip(0.049804688 + 0.89941406 * jax.random.uniform(part_splits[3], (SLOT_TOTAL, 2), jnp.float32) ** block_levels(part_splits[3], (SLOT_TOTAL, 2), ((0, 128),), -0.2, 0.2), 0.049804688, 0.94921875).astype(jnp.bfloat16)
    slot_sigma = jnp.clip(jnp.exp(math.log(2.0) - 1.3862944 * jax.random.uniform(part_splits[4], (SLOT_TOTAL, BAND_COUNT), jnp.float32) ** block_levels(part_splits[4], (SLOT_TOTAL, BAND_COUNT), ((0, 128), (1, 2)), -0.2, 0.2)), 0.5, 2.0).astype(jnp.bfloat16)
    clip_mask = plant((jax.random.randint(part_splits[5], (SLOT_TOTAL, (ROWS_DEV + 2 * MARGIN) // 8, TILE_COLS // 32), 0, 8) < 7).astype(jnp.int32), jax.random.fold_in(part_splits[5], 1), 0, 1)
    slot_count = plant(jax.random.randint(part_splits[6], (N_SKY * N_EPOCH,), 3 * SLOT_DEV // 4, SLOT_DEV + 1), jax.random.fold_in(part_splits[6], 1), 3 * SLOT_DEV // 4, SLOT_DEV).astype(jnp.int32)
    template = gaussian(part_splits[7], (BAND_COUNT, PATCH_ROWS, TILE_COLS), 1.0, 6.0, ((0, 2), (1, 32)))
    prior_weight = jnp.clip(jnp.exp(math.log(4.0) - 2.0794415 * jax.random.uniform(part_splits[8], (BAND_COUNT, PATCH_ROWS), jnp.float32) ** block_levels(part_splits[8], (BAND_COUNT, PATCH_ROWS), ((0, 2), (1, 32)), -0.2, 0.2)), 0.5, 4.0)
    return {"slot_pixels": slot_pixels, "slot_tile": slot_tile, "slot_offset": slot_offset, "slot_frac": slot_frac, "slot_sigma": slot_sigma, "clip_mask": clip_mask, "slot_count": slot_count, "template": template, "prior_weight": prior_weight}


CLIP_WIDTH = 3.0


def lanczos(distance):
    inside = jnp.abs(distance) < 3.0
    return jnp.where(inside, jnp.sinc(distance) * jnp.sinc(distance / 3.0), 0.0)


def tap_weights(fraction):
    steps_back = jnp.arange(-3, 3, dtype=jnp.int32)
    distance = (-steps_back).astype(jnp.float32) - fraction
    rounded = lanczos(distance).astype(jnp.bfloat16)
    return lax.optimization_barrier(rounded).astype(jnp.float32)


def reference(slot_pixels, slot_tile, slot_offset, slot_frac, slot_sigma, clip_mask, slot_count, template, prior_weight):
    slot_number = slot_pixels.shape[0]
    canvas_rows = ROWS_DEV + 2 * MARGIN
    patch_rows = template.shape[1]
    tile_cols = template.shape[2]
    template_pad = jnp.pad(template.astype(jnp.float32), ((0, 0), (MARGIN, MARGIN), (0, 0)))
    empty_sums = jnp.zeros((BAND_COUNT, patch_rows + 2 * MARGIN, tile_cols), jnp.float32)
    row_index = jnp.arange(canvas_rows, dtype=jnp.int32)
    col_index = jnp.arange(tile_cols, dtype=jnp.int32)

    def one_slot(carried, slot_index):
        flux_sums, weight_sums = carried
        pixels = lax.dynamic_index_in_dim(slot_pixels, slot_index, 0, keepdims=False).astype(jnp.float32)
        tile_index = slot_tile[slot_index, 0]
        shift_y = slot_offset[slot_index, 0]
        shift_x = slot_offset[slot_index, 1]
        taps_y = tap_weights(slot_frac[slot_index, 0].astype(jnp.float32))
        taps_x = tap_weights(slot_frac[slot_index, 1].astype(jnp.float32))
        is_live = ((slot_index % SLOT_DEV) < slot_count[slot_index // SLOT_DEV]).astype(jnp.float32)
        padded = jnp.pad(pixels, ((0, 0), (0, 0), (MARGIN, MARGIN)))
        columns = jnp.zeros((BAND_COUNT, ROWS_DEV, tile_cols), jnp.float32)
        col_cover = jnp.zeros((tile_cols,), jnp.float32)
        for tap_index in range(6):
            step_back = tap_index - 3
            shifted = lax.dynamic_slice_in_dim(padded, MARGIN - shift_x + step_back, tile_cols, 2)
            columns = columns + taps_x[tap_index] * shifted
            source_col = col_index - shift_x + step_back
            inside = (source_col >= 0) & (source_col < tile_cols)
            col_cover = col_cover + jnp.where(inside, taps_x[tap_index], 0.0)
        columns = lax.optimization_barrier(columns.astype(jnp.bfloat16)).astype(jnp.float32)
        column_pad = jnp.pad(columns, ((0, 0), (2 * MARGIN, 2 * MARGIN), (0, 0)))
        warped = jnp.zeros((BAND_COUNT, canvas_rows, tile_cols), jnp.float32)
        row_cover = jnp.zeros((canvas_rows,), jnp.float32)
        for tap_index in range(6):
            step_back = tap_index - 3
            shifted = lax.dynamic_slice_in_dim(column_pad, MARGIN - shift_y + step_back, canvas_rows, 1)
            warped = warped + taps_y[tap_index] * shifted
            source_row = row_index - MARGIN - shift_y + step_back
            inside = (source_row >= 0) & (source_row < ROWS_DEV)
            row_cover = row_cover + jnp.where(inside, taps_y[tap_index], 0.0)
        row_cover = jnp.clip(row_cover, 0.0, 1.0)
        col_cover = jnp.clip(col_cover, 0.0, 1.0)
        block_mask = clip_mask[slot_index].astype(jnp.float32)
        expanded = jnp.repeat(jnp.repeat(block_mask, 8, axis=0), 32, axis=1) * is_live
        plane = (expanded * row_cover[:, None]) * col_cover[None, :]
        sigmas = slot_sigma[slot_index].astype(jnp.float32)
        weight = plane[None] / (sigmas * sigmas)[:, None, None]
        framed = lax.dynamic_slice_in_dim(template_pad, tile_index * ROWS_DEV, canvas_rows, 1)
        scale = CLIP_WIDTH * sigmas[:, None, None]
        clipped = framed + scale * jnp.tanh((warped - framed) / scale)
        start = tile_index * ROWS_DEV
        old_flux = lax.dynamic_slice_in_dim(flux_sums, start, canvas_rows, 1)
        old_weight = lax.dynamic_slice_in_dim(weight_sums, start, canvas_rows, 1)
        flux_sums = lax.dynamic_update_slice_in_dim(flux_sums, old_flux + weight * clipped, start, 1)
        weight_sums = lax.dynamic_update_slice_in_dim(weight_sums, old_weight + weight, start, 1)
        return (flux_sums, weight_sums), None

    (flux_sums, weight_sums), _ = lax.scan(one_slot, (empty_sums, empty_sums), jnp.arange(slot_number, dtype=jnp.int32))
    flux_sum = flux_sums[:, MARGIN:MARGIN + patch_rows]
    weight_sum = weight_sums[:, MARGIN:MARGIN + patch_rows]
    prior = prior_weight[:, :, None]
    coadd_image = ((flux_sum + prior * template.astype(jnp.float32)) / (weight_sum + prior)).astype(jnp.bfloat16)
    depth_map = weight_sum + prior
    band_mean = jnp.sum(depth_map, axis=(1, 2)) / (patch_rows * tile_cols)
    depth_norm = (depth_map / band_mean[:, None, None]).astype(jnp.bfloat16)
    return coadd_image, depth_norm
```

```python
import functools
import math

import jax
import jax.numpy as jnp
from jax import lax
from jax.experimental import pallas as pl
from jax.experimental.pallas import tpu as pltpu
from jax.sharding import PartitionSpec as P

MESH = pl.DeviceIdType.MESH
MARGIN = 8
CLIP_WIDTH = 3.0
TAPS = tuple(range(-2, 4))
EDGE = 8
BLOCK = 32
LANES = 128


def iota(shape, dim):
    return lax.broadcasted_iota(jnp.int32, shape, dim)


def tap_values(fraction):
    sin_whole = jnp.sin(math.pi * fraction)
    sin_third = jnp.sin((math.pi / 3.0) * fraction)
    cos_third = jnp.cos((math.pi / 3.0) * fraction)
    values = []
    for d in TAPS:
        u = d - fraction
        top = -math.cos(math.pi * d) * sin_whole
        third = math.sin(math.pi * d / 3.0) * cos_third - math.cos(math.pi * d / 3.0) * sin_third
        value = top * third / ((math.pi * math.pi / 3.0) * u * u)
        value = jnp.where(jnp.abs(u) < 3.0, value, 0.0)
        values.append(value.astype(jnp.bfloat16).astype(jnp.float32))
    return values


def tap_select(gap, taps):
    value = jnp.zeros(gap.shape, jnp.float32)
    for d, tap in zip(TAPS, taps):
        value = jnp.where(gap == d, tap, value)
    return value


def greet(peers):
    barrier = pltpu.get_barrier_semaphore()
    for peer in peers:
        pl.semaphore_signal(barrier, inc=1, device_id=peer, device_id_type=MESH)
    pl.semaphore_wait(barrier, len(peers))


def places(n, ne):
    me = lax.axis_index("sky")
    e = lax.axis_index("epoch")

    def sky(shift):
        return lax.rem(me + shift + n, n)

    def epoch(shift):
        return lax.rem(e + shift + ne, ne)

    return sky, epoch


def remote(src, dst, send_sem, recv_sem, peer):
    return pltpu.make_async_remote_copy(
        src_ref=src, dst_ref=dst, send_sem=send_sem, recv_sem=recv_sem, device_id=peer, device_id_type=MESH
    )


def gather_kernel(
    n, ne, offset, pix_hbm, frac_ref, sigma_ref, mask_ref, tmpl_hbm, warped_hbm, cover_hbm, mc_hbm, all_hbm,
    pix, warped, cover, mc, held, kx, taps, squares,
    in_sem, chain_send, chain_recv, fan_send, fan_recv, x_send, x_recv, out_sem, slot_sem, mc_sem,
):
    slots, lines, width = pix.shape
    bands, rows = held.shape[2], held.shape[3]
    canvas = rows + 2 * MARGIN
    steps = n // 4
    per_step = slots // steps
    sky, epoch = places(n, ne)
    me = sky(0)
    load_pix = pltpu.make_async_copy(pix_hbm, pix, in_sem.at[0])

    def load_own(q):
        return pltpu.make_async_copy(
            tmpl_hbm.at[:, :, pl.ds(q * LANES, LANES)], held.at[me, q], in_sem.at[1 + q]
        )

    for q in range(ne):
        load_own(q).start()
    load_pix.start()
    greet([{"sky": sky(k)} for k in (-2, -1, 1, 2)] + [{"epoch": epoch(k)} for k in (-1, 1)])
    for q in range(ne):
        load_own(q).wait()

    def quarter(c):
        return epoch(c)

    def block(side, distance):
        return sky(-distance if side == 0 else distance)

    def chain(side, j, c):
        piece = held.at[block(side, 2 * j), quarter(c)]
        return remote(
            piece, piece, chain_send.at[side, j, c], chain_recv.at[side, j, c],
            {"sky": sky(2 if side == 0 else -2)},
        )

    def fan(side, j, c):
        piece = held.at[block(side, 2 * j), quarter(c)]
        return remote(
            piece, piece, fan_send.at[side, j, c], fan_recv.at[side, j, c],
            {"sky": sky(1 if side == 0 else -1)},
        )

    def across(owner, c):
        piece = held.at[owner, quarter(c)]
        return remote(
            piece, piece, x_send.at[c, owner], x_recv.at[c, owner], {"epoch": epoch(1 if c == 0 else -1)}
        )

    for c in (0, 1):
        for side in (0, 1):
            chain(side, 0, c).start()
    for c in (0, 1):
        for side in (0, 1):
            fan(side, 0, c).start()

    lanes = mc.shape[2]
    lane = iota((16, lanes), 1)
    tail = lane - width
    inner = lax.rem(tail, 32)
    chosen = jnp.where(
        tail < 0,
        lane // BLOCK,
        jnp.where(inner < 16, inner, jnp.where(inner < 24, 0, 15)),
    )
    spread = jnp.where((chosen == iota((16, lanes), 0)) & (tail < bands * 32), 1.0, 0.0).astype(jnp.bfloat16)
    kx[...] = jnp.zeros_like(kx)
    fractions = frac_ref[...].astype(jnp.float32)
    for axis in (0, 1):
        wide = jnp.broadcast_to(fractions[:, axis : axis + 1], (slots, LANES))
        for i, value in enumerate(tap_values(wide)):
            taps[axis * len(TAPS) + i] = value
    sigma = sigma_ref[...].astype(jnp.float32)
    band_of = iota((slots, LANES), 1) // 32
    square = jnp.zeros((slots, LANES), jnp.float32)
    for b in range(bands):
        s = jnp.broadcast_to(sigma[:, b : b + 1], (slots, LANES))
        square = jnp.where(band_of == b, 1.0 / (s * s), square)
    squares[...] = square
    load_pix.wait()
    ones = jnp.ones((rows, LANES), jnp.bfloat16)

    def warp(slot, table):
        dy = offset[slot, 0]
        dx = offset[slot, 1]
        row_taps = [taps[i, pl.ds(slot, 1), :] for i in range(6)]
        col_taps = [taps[6 + i, pl.ds(slot, 1), :] for i in range(6)]
        lead = (LANES, LANES)
        middle = tap_select(iota(lead, 1) - iota(lead, 0) - dx, col_taps).astype(jnp.bfloat16)
        rim = (16, LANES)
        gap = iota(rim, 1) - iota(rim, 0) - dx
        above = tap_select(gap + 16, col_taps).astype(jnp.bfloat16)
        below = tap_select(gap - LANES, col_taps).astype(jnp.bfloat16)
        blocks = width // LANES
        for jb in range(blocks):
            span = slice(jb * LANES, (jb + 1) * LANES)
            table[span, span] = middle
            if jb > 0:
                table[jb * LANES - 16 : jb * LANES, span] = above
            if jb < blocks - 1:
                table[(jb + 1) * LANES : (jb + 1) * LANES + 16, span] = below
        columns = jnp.dot(pix[slot], table[...], preferred_element_type=jnp.float32).astype(jnp.bfloat16)
        shape = (canvas, LANES)
        gap = iota(shape, 0) - MARGIN - dy - iota(shape, 1)
        row_table = tap_select(gap, row_taps)[:, :rows].astype(jnp.bfloat16)
        for b in range(bands):
            warped[slot, b * canvas : (b + 1) * canvas] = jnp.dot(
                row_table, columns[b * rows : (b + 1) * rows], preferred_element_type=jnp.float32
            ).astype(jnp.bfloat16)
        cover[slot] = jnp.clip(jnp.dot(row_table, ones, preferred_element_type=jnp.float32), 0.0, 1.0)
        shape = (8, lanes)
        at = iota(shape, 1)
        over = at - width
        part = lax.rem(over, 32)
        column = jnp.where(
            over < 0,
            at,
            jnp.where(part < 16, 256, jnp.where(part < 24, part - 16, width - 32 + part)),
        )
        col_cover = jnp.zeros(shape, jnp.float32)
        for d, tap in zip(TAPS, col_taps):
            source = column - dx - d
            tap = jnp.concatenate([tap] * (lanes // LANES), axis=1)
            col_cover = col_cover + jnp.where((source >= 0) & (source < width), tap, 0.0)
        col_cover = jnp.clip(col_cover, 0.0, 1.0)
        mask_rows = mask_ref.shape[1]
        mask = mask_ref[slot].astype(jnp.float32).astype(jnp.bfloat16)
        planes = jnp.dot(mask, spread, preferred_element_type=jnp.float32) * col_cover[:mask_rows]
        mc[slot, 0:mask_rows, 0:width] = planes[:, :width]
        mc[slot, 0:mask_rows, width:] = planes[:, width:] * squares[pl.ds(slot, 1), :]

    def store_out(owner):
        return pltpu.make_async_copy(held.at[owner], all_hbm.at[owner], out_sem.at[owner])

    def slots_out(step):
        which = pl.ds(step * per_step, per_step)
        return (
            pltpu.make_async_copy(warped.at[which], warped_hbm.at[which], slot_sem.at[0, step]),
            pltpu.make_async_copy(cover.at[which], cover_hbm.at[which], slot_sem.at[1, step]),
        )

    def body(j, stage):
        for c in (0, 1):
            chain(0, j - 1, c).wait_recv()
            if stage < 2:
                chain(0, j, c).start()
                chain(1, j - 1, c).wait_recv()
            if stage < 1:
                chain(1, j, c).start()
            if stage < 2:
                for side in (0, 1):
                    fan(side, j, c).start()
            across(block(0, 2 * j), c).start()
            if stage < 2:
                across(block(1, 2 * j), c).start()
        for c in (0, 1):
            for side in (0, 1):
                fan(side, j - 1, c).wait_recv()
                across(block(side, 2 * j - 1), c).start()

        @pl.loop((j - 1) * per_step, j * per_step)
        def _(slot):
            warp(slot, kx)

        for copy in slots_out(j - 1):
            copy.start()

    @pl.loop(1, steps - 1)
    def _(j):
        body(j, 0)

    body(steps - 1, 1)
    body(steps, 2)
    mc_out = pltpu.make_async_copy(mc, mc_hbm, mc_sem.at[0])
    mc_out.start()
    store_out(me).start()

    @pl.loop(1, n)
    def _(k):
        owner = sky(k)
        for c in (0, 1):
            across(owner, c).wait_recv()
        store_out(owner).start()

    @pl.loop(1, n)
    def _(k):
        owner = sky(k)
        for c in (0, 1):
            across(owner, c).wait_send()
        store_out(owner).wait()

    store_out(me).wait()

    @pl.loop(0, steps)
    def _(j):
        for c in (0, 1):
            chain(0, j, c).wait_send()
            for side in (0, 1):
                fan(side, j, c).wait_send()
        for copy in slots_out(j):
            copy.wait()

    @pl.loop(0, steps - 1)
    def _(j):
        for c in (0, 1):
            chain(1, j, c).wait_send()

    mc_out.wait()


def accumulate_kernel(
    ne, tile, count, warped_hbm, cover_hbm, mc_hbm, all_hbm, sigma_ref, prior_ref, part_hbm, wpart_hbm, total_ref,
    warped, cover, mc, tmpl, framed, flux, wsum, wout, scales, slot_sem, sem,
):
    slots, width = warped.shape[0], warped.shape[2]
    n, quarters, bands, rows = tmpl.shape[:4]
    canvas = rows + 2 * MARGIN
    pieces = slot_sem.shape[1]
    piece = slots // pieces
    load_tmpl = pltpu.make_async_copy(all_hbm, tmpl, sem.at[0])
    load_mc = pltpu.make_async_copy(mc_hbm, mc, sem.at[1])

    def load_slots(q):
        which = pl.ds(q * piece, piece)
        return (
            pltpu.make_async_copy(warped_hbm.at[which], warped.at[which], slot_sem.at[0, q]),
            pltpu.make_async_copy(cover_hbm.at[which], cover.at[which], slot_sem.at[1, q]),
        )

    load_tmpl.start()
    load_mc.start()
    for q in range(pieces):
        for copy in load_slots(q):
            copy.start()

    sigma = sigma_ref[...].astype(jnp.float32)
    for b in range(bands):
        s = jnp.broadcast_to(sigma[:, b : b + 1], (slots, LANES))
        scales[b] = CLIP_WIDTH * s
        scales[bands + b] = 1.0 / (CLIP_WIDTH * s)
        scales[2 * bands + b] = 1.0 / (s * s)

    @pl.loop(0, n)
    def _(t):
        at = pl.ds(pl.multiple_of(t * rows, rows), rows)
        for b in range(bands):
            flux[b, at, :] = jnp.zeros((rows, width), jnp.float32)
        wsum[at, :] = jnp.zeros((rows, LANES), jnp.float32)

    total_rows = flux.shape[1]
    ends = total_rows - n * rows
    for b in range(bands):
        flux[b, n * rows :, :] = jnp.zeros((ends, width), jnp.float32)
        framed[b, 0:MARGIN, :] = jnp.zeros((MARGIN, width), jnp.float32)
        framed[b, total_rows - MARGIN :, :] = jnp.zeros((MARGIN, width), jnp.float32)
    wsum[n * rows :, :] = jnp.zeros((ends, LANES), jnp.float32)
    load_tmpl.wait()

    @pl.loop(0, n)
    def _(t):
        at = pl.ds(pl.multiple_of(t * rows + MARGIN, MARGIN), rows)
        for b in range(bands):
            for q in range(quarters):
                framed[b, at, q * LANES : (q + 1) * LANES] = tmpl[t, q, b].astype(jnp.float32)

    load_mc.wait()
    live = count[0]
    mask_rows = canvas // 8

    def spread(block):
        wide = block.shape[1]
        return jnp.broadcast_to(block[:, None, :], (mask_rows, 8, wide)).reshape(canvas, wide)

    def one(p):
        row0 = pl.multiple_of(tile[p, 0] * rows, rows)
        at = pl.ds(row0, canvas)
        rim = cover[p]
        scale = [scales[i, pl.ds(p, 1), :] for i in range(3 * bands)]
        for q in range(width // LANES):
            span = pl.ds(q * LANES, LANES)
            plane = spread(mc[p, 0:mask_rows, span]) * rim
            for b in range(bands):
                frame = framed[b, at, span]
                moved = warped[p, pl.ds(b * canvas, canvas), span].astype(jnp.float32)
                moved = jnp.tanh((moved - frame) * scale[bands + b])
                flux[b, at, span] += (plane * scale[2 * bands + b]) * (frame + scale[b] * moved)
        wsum[at, :] += spread(mc[p, 0:mask_rows, pl.ds(width, LANES)]) * rim

    for q in range(pieces):
        for copy in load_slots(q):
            copy.wait()

        @pl.loop(q * piece, jnp.minimum(live, (q + 1) * piece))
        def _(p):
            one(p)

    def add_rows(t, total):
        at = pl.ds(pl.multiple_of(t * rows + MARGIN, MARGIN), rows)
        block = wsum[at, :]
        for g in range(ne):
            wout[g, t] = block[g * 8 : (g + 1) * 8]
        for b in range(bands):
            for q in range(quarters):
                tmpl[t, q, b] = flux[b, at, q * LANES : (q + 1) * LANES].astype(jnp.bfloat16)
        return total + sum(block[i : i + 8] for i in range(0, rows, 8))

    total = lax.fori_loop(0, n, add_rows, jnp.zeros((8, LANES), jnp.float32))
    part_out = pltpu.make_async_copy(tmpl, part_hbm, sem.at[0])
    part_out.start()
    w_out = pltpu.make_async_copy(wout, wpart_hbm, sem.at[1])
    w_out.start()
    lane = iota((8, LANES), 1)
    inner = lax.rem(lane, 32)
    times = jnp.where(
        lane >= bands * 32,
        0.0,
        jnp.where(
            inner >= 16,
            1.0,
            jnp.where((inner == 0) | (inner == 15), float(BLOCK - EDGE), float(BLOCK)),
        ),
    )
    total = jnp.broadcast_to(jnp.sum(total, axis=0, keepdims=True), (8, LANES)) * times
    for b in range(bands):
        prior = jnp.sum(prior_ref[b : b + 1, :], axis=1, keepdims=True) * (width / ne)
        total = total + jnp.where(lane == b * 32, prior, 0.0)
    total_ref[...] = total
    part_out.wait()
    w_out.wait()


def reduce_kernel(
    n, ne, part_hbm, wpart_hbm, total_ref, tmpl_ref, prior_ref, image_ref, norm_ref,
    part, wpart, xin, xwin, xtin, shared, chain_out, wchain_out, chain_in, wchain_in,
    fan_out, wfan_out, fan_in, wfan_in, half_out, half_in, kept,
    load_sem, x_send, x_recv, xw_sem, xt_sem, chain_send, chain_recv, fan_send, fan_recv, half_sem, kept_sem,
):
    bands, rows = part.shape[2:4]
    width = ne * LANES
    steps = n // 4
    sky, epoch = places(n, ne)
    e = epoch(0)

    def step_owners(s):
        i = steps - s
        return (sky(2 * i), sky(-2 * i), sky(2 * i - 1), sky(1 - 2 * i))

    def load(c):
        return pltpu.make_async_copy(part_hbm.at[:, epoch(c)], part.at[c], load_sem.at[c])

    load_w = pltpu.make_async_copy(wpart_hbm.at[e], wpart, load_sem.at[2])
    for c in (0, 1):
        load(c).start()
    load_w.start()
    greet([{"sky": sky(k)} for k in (-2, -1, 1, 2)] + [{"epoch": epoch(k)} for k in range(1, ne)])

    def cross(owner, c):
        return remote(
            part_hbm.at[owner, epoch(-1 if c == 0 else 2)],
            xin.at[c, owner],
            x_send.at[c, owner],
            x_recv.at[c, owner],
            {"epoch": epoch(-1 if c == 0 else 1)},
        )

    def cross_w(k):
        peer = epoch(k)
        return remote(
            wpart_hbm.at[peer], xwin.at[k - 1], xw_sem.at[0, k - 1], xw_sem.at[1, k - 1], {"epoch": peer}
        )

    def cross_t(k):
        return remote(
            total_ref, xtin.at[k - 1], xt_sem.at[0, k - 1], xt_sem.at[1, k - 1], {"epoch": epoch(k)}
        )

    def cross_owners(owners):
        for owner in owners:
            for c in (0, 1):
                cross(owner, c).start()

    first = step_owners(0)
    cross_owners((first[0], first[2], first[3]))
    for k in range(1, ne):
        cross_t(k).start()
        cross_w(k).start()

    @pl.loop(1, steps)
    def _(s):
        cross_owners(step_owners(s))

    cross_owners((sky(0),))

    def chain(side, s, c):
        whole = c < 2
        return remote(
            chain_out.at[side, s, c] if whole else wchain_out.at[side, s],
            chain_in.at[side, s, c] if whole else wchain_in.at[side, s],
            chain_send.at[side, s, c],
            chain_recv.at[side, s, c],
            {"sky": sky(2 if side == 0 else -2)},
        )

    def fan(side, k, c):
        whole = c < 2
        return remote(
            fan_out.at[side, k, c] if whole else wfan_out.at[side, k],
            fan_in.at[side, k, c] if whole else wfan_in.at[side, k],
            fan_send.at[side, k, c],
            fan_recv.at[side, k, c],
            {"sky": sky(1 if side == 0 else -1)},
        )

    def own(owner, c):
        if c < 2:
            return part[c, owner].astype(jnp.float32) + xin[c, owner].astype(jnp.float32)
        block = wpart[owner]
        for k in range(1, ne):
            block = block + xwin[k - 1, owner]
        return jnp.concatenate([block, shared[...]], axis=0)

    def received(kind, side, k, c):
        if c < 2:
            return (chain_in if kind == 0 else fan_in)[side, k, c].astype(jnp.float32)
        return (wchain_in if kind == 0 else wfan_in)[side, k]

    def wait_cross(owner):
        for c in (0, 1):
            cross(owner, c).wait_recv()

    def chain_step(s, side, has_chain, has_fan):
        i = steps - s
        owner = sky(2 * i if side == 0 else -2 * i)
        for c in range(3):
            if has_chain:
                chain(side, s - 1, c).wait_recv()
            if has_fan:
                fan(side, i, c).wait_recv()
            value = own(owner, c)
            if has_chain:
                value = value + received(0, side, s - 1, c)
            if has_fan:
                value = value + received(1, side, i, c)
            if c < 2:
                chain_out[side, s, c] = value.astype(jnp.bfloat16)
            else:
                wchain_out[side, s] = value
            chain(side, s, c).start()

    def fan_step(s, side):
        k = steps - s - 1
        owner = sky(2 * k + 1 if side == 0 else -2 * k - 1)
        wait_cross(owner)
        for c in range(3):
            value = own(owner, c)
            if c < 2:
                fan_out[side, k, c] = value.astype(jnp.bfloat16)
            else:
                wfan_out[side, k] = value
            fan(side, k, c).start()

    for c in (0, 1):
        load(c).wait()
    load_w.wait()
    for k in range(1, ne):
        cross_t(k).wait_recv()
        cross_w(k).wait_recv()
    gathered = total_ref[...]
    for k in range(1, ne):
        gathered = gathered + xtin[k - 1]
    shared[...] = gathered

    wait_cross(first[0])
    chain_step(0, 0, False, False)
    for side in (0, 1):
        fan_step(0, side)
    for side in (0, 1):
        wait_cross(sky(2 * (steps - 1) if side == 0 else -2 * (steps - 1)))
        chain_step(1, side, side == 0, True)
    for side in (0, 1):
        fan_step(1, side)

    @pl.loop(2, steps)
    def _(s):
        i = steps - s
        for side in (0, 1):
            wait_cross(sky(2 * i if side == 0 else -2 * i))
            chain_step(s, side, True, True)
        for side in (0, 1):
            fan_step(s, side)

    me = sky(0)
    wait_cross(me)
    sums = []
    for c in (1, 2, 0):
        value = own(me, c)
        for side in (0, 1):
            fan(side, 0, c).wait_recv()
            value = value + received(1, side, 0, c)
        for side in (0, 1):
            chain(side, steps - 1, c).wait_recv()
            value = value + received(0, side, steps - 1, c)
        if c == 1:
            half_out[...] = value.astype(jnp.bfloat16)
            half = remote(half_out, half_in, half_sem.at[0], half_sem.at[1], {"epoch": epoch(1)})
            half.start()
        elif c == 2:
            kept[e] = value[0:8]
            total = value[8:9]

            def keep(k):
                return remote(
                    kept.at[e], kept.at[e], kept_sem.at[0, k - 1], kept_sem.at[1, k - 1], {"epoch": epoch(k)}
                )

            for k in range(1, ne):
                keep(k).start()
        else:
            mine = value

    lane = iota((LANES, LANES), 1) + e * LANES
    row = iota((LANES, LANES), 0)
    inner = jnp.where(
        lane < EDGE, 16 + lane, jnp.where(lane >= width - EDGE, lane - (width - 32), lane // BLOCK)
    )
    here = pl.ds(pl.multiple_of(e * LANES, LANES), LANES)
    lane1 = iota((1, LANES), 1)
    eye = iota((rows, rows), 0) == iota((rows, rows), 1)
    half.wait()
    for k in range(1, ne):
        keep(k).wait()
    weights = kept[...].reshape(rows, LANES)
    for b in range(bands):
        pick = jnp.where(row == inner + b * 32, 1.0, 0.0)
        weight = jnp.dot(
            weights, pick, preferred_element_type=jnp.float32, precision=lax.Precision.HIGHEST
        )
        prior = jnp.sum(
            jnp.where(eye, jnp.broadcast_to(prior_ref[b : b + 1, :], (rows, rows)), 0.0), axis=1, keepdims=True
        )
        depth = weight + prior
        base = tmpl_ref[b, :, here].astype(jnp.float32)
        image_ref[b] = (mine[b] + half_in[b].astype(jnp.float32) + prior * base) / depth
        band = jnp.sum(jnp.where(lane1 // 32 == b, total, 0.0), axis=1, keepdims=True)
        norm_ref[b] = depth / (band / float(rows * n * width))

    @pl.loop(0, n)
    def _(k):
        for c in (0, 1):
            cross(sky(k), c).wait_send()

    for k in range(1, ne):
        cross_w(k).wait_send()
        cross_t(k).wait_send()

    @pl.loop(0, steps)
    def _(s):
        for c in range(3):
            chain(0, s, c).wait_send()
            for side in (0, 1):
                fan(side, s, c).wait_send()

    @pl.loop(1, steps)
    def _(s):
        for c in range(3):
            chain(1, s, c).wait_send()


def on_device(
    slot_pixels,
    slot_tile,
    slot_offset,
    slot_frac,
    slot_sigma,
    clip_mask,
    slot_count,
    template,
    prior_weight,
):
    n = lax.axis_size("sky")
    ne = lax.axis_size("epoch")
    steps = n // 4
    slots, bands, rows, width = slot_pixels.shape
    canvas = rows + 2 * MARGIN
    lanes = width + LANES
    smem = pl.BlockSpec(memory_space=pltpu.SMEM)
    vmem = pl.BlockSpec(memory_space=pltpu.VMEM)
    hbm = pl.BlockSpec(memory_space=pl.ANY)
    dma = pltpu.SemaphoreType.DMA
    bf16, f32 = jnp.bfloat16, jnp.float32
    warped_type = jax.ShapeDtypeStruct((slots, bands * canvas, width), bf16)
    cover_type = jax.ShapeDtypeStruct((slots, canvas, LANES), f32)
    mc_type = jax.ShapeDtypeStruct((slots, 8, lanes), f32)
    blocks_type = jax.ShapeDtypeStruct((n, ne, bands, rows, LANES), bf16)

    def like(shape):
        return pltpu.VMEM(shape.shape, shape.dtype)

    warped, cover, mc, gathered = pl.pallas_call(
        functools.partial(gather_kernel, n, ne),
        out_shape=(warped_type, cover_type, mc_type, blocks_type),
        in_specs=[smem, hbm, vmem, vmem, vmem, hbm],
        out_specs=(hbm, hbm, hbm, hbm),
        scratch_shapes=[
            pltpu.VMEM((slots, bands * rows, width), bf16),
            like(warped_type),
            like(cover_type),
            like(mc_type),
            like(blocks_type),
            pltpu.VMEM((width, width), bf16),
            pltpu.VMEM((2 * len(TAPS), slots, LANES), f32),
            pltpu.VMEM((slots, LANES), f32),
            dma((1 + ne,)),
            dma((2, steps, 2)),
            dma((2, steps, 2)),
            dma((2, steps, 2)),
            dma((2, steps, 2)),
            dma((2, n)),
            dma((2, n)),
            dma((n,)),
            dma((2, steps)),
            dma((1,)),
        ],
        compiler_params=pltpu.CompilerParams(collective_id=0, has_side_effects=True),
        name="gather",
    )(slot_offset, slot_pixels.reshape(slots, bands * rows, width), slot_frac, slot_sigma, clip_mask, template)

    padded = n * rows + 2 * MARGIN
    wpart_type = jax.ShapeDtypeStruct((ne, n, 8, LANES), f32)
    total_type = jax.ShapeDtypeStruct((8, LANES), f32)
    part, wpart, total = pl.pallas_call(
        functools.partial(accumulate_kernel, ne),
        out_shape=(blocks_type, wpart_type, total_type),
        in_specs=[smem, smem, hbm, hbm, hbm, hbm, vmem, vmem],
        out_specs=(hbm, hbm, vmem),
        scratch_shapes=[
            like(warped_type),
            like(cover_type),
            like(mc_type),
            like(blocks_type),
            pltpu.VMEM((bands, padded, width), f32),
            pltpu.VMEM((bands, padded, width), f32),
            pltpu.VMEM((padded, LANES), f32),
            like(wpart_type),
            pltpu.VMEM((3 * bands, slots, LANES), f32),
            dma((2, 6)),
            dma((2,)),
        ],
        name="accumulate",
    )(slot_tile, slot_count, warped, cover, mc, gathered, slot_sigma, prior_weight)

    half_type = (bands, rows, LANES)
    out = jax.ShapeDtypeStruct((bands, rows, width // ne), f32)
    image, norm = pl.pallas_call(
        functools.partial(reduce_kernel, n, ne),
        out_shape=(out, out),
        in_specs=[hbm, hbm, vmem, vmem, vmem],
        out_specs=(vmem, vmem),
        scratch_shapes=[
            pltpu.VMEM((2, n) + half_type, bf16),
            pltpu.VMEM((n, 8, LANES), f32),
            pltpu.VMEM((2, n) + half_type, bf16),
            pltpu.VMEM((ne - 1, n, 8, LANES), f32),
            pltpu.VMEM((ne - 1, 8, LANES), f32),
            pltpu.VMEM((8, LANES), f32),
            pltpu.VMEM((2, steps, 2) + half_type, bf16),
            pltpu.VMEM((2, steps, 16, LANES), f32),
            pltpu.VMEM((2, steps, 2) + half_type, bf16),
            pltpu.VMEM((2, steps, 16, LANES), f32),
            pltpu.VMEM((2, steps, 2) + half_type, bf16),
            pltpu.VMEM((2, steps, 16, LANES), f32),
            pltpu.VMEM((2, steps, 2) + half_type, bf16),
            pltpu.VMEM((2, steps, 16, LANES), f32),
            pltpu.VMEM(half_type, bf16),
            pltpu.VMEM(half_type, bf16),
            pltpu.VMEM((ne, 8, LANES), f32),
            dma((3,)),
            dma((2, n)),
            dma((2, n)),
            dma((2, ne - 1)),
            dma((2, ne - 1)),
            dma((2, steps, 3)),
            dma((2, steps, 3)),
            dma((2, steps, 3)),
            dma((2, steps, 3)),
            dma((2,)),
            dma((2, ne - 1)),
        ],
        compiler_params=pltpu.CompilerParams(collective_id=1, has_side_effects=True),
        name="reduce",
    )(part, wpart, total, template, prior_weight)
    return (image.astype(bf16), norm.astype(bf16))


def solution(mesh):
    in_specs = (
        P(("groups", "sky", "epoch"), "band", None, None),
        P(("groups", "sky", "epoch"), None),
        P(("groups", "sky", "epoch"), None),
        P(("groups", "sky", "epoch"), None),
        P(("groups", "sky", "epoch"), "band"),
        P(("groups", "sky", "epoch"), None, None),
        P(("groups", "sky", "epoch")),
        P("band", ("groups", "sky"), None),
        P("band", ("groups", "sky")),
    )
    out_specs = (P("band", ("groups", "sky"), "epoch"), P("band", ("groups", "sky"), "epoch"))
    return jax.shard_map(
        on_device, mesh=mesh, in_specs=in_specs, out_specs=out_specs, check_vma=False
    )
```
